32 devices in a mesh: vis: 8 (over z, x), tile: 4 (over y, core).
Axes of the slice: x: 2, y: 2, z: 4, core: 2. Of those that a mesh axis runs over, the one named last changes fastest.
Arguments:
- spectra: bfloat16 [64, 2048], P(None, ('vis', 'tile')), may hold values from -0.1875 to 0.1875
- positions: int32 [2, 2048], P(None, ('vis', 'tile')), may hold values from 0 to 8191
- observed: bfloat16 [32768, 128], P(('vis', 'tile')), may hold values from -6 to 6
- cells: int32 [2, 32768], P(None, ('vis', 'tile')), may hold values from 0 to 8184, as said below
- fractions: float32 [2, 32768], P(None, ('vis', 'tile')), may hold values from 0 to 1
- bucket_counts: int32 [32, 4], P(('vis', 'tile')), may hold values from 0 to 512, as said below
- chan_weights: float32 [64], replicated, may hold values from 0.04 to 0.32
Outputs:
- residual_vis: bfloat16 [32768, 128], P(('vis', 'tile'))
- residual_grid: float32 [128, 2, 8192], P('vis', None, 'tile')
The draws below stay inside these ranges and needn't reach their ends.
Inputs may be any that keep to these rules, and one draw needn't show every extreme that they name: cells[0, r] is the first uv column and cells[1, r] the first uv row of row r's 8 x 8 kernel window, with cells[1, r] <= 120. The rows of each device are ordered by tile: for device d and tile t, the bucket_counts[d, t] rows that start after the first sum of bucket_counts[d, 0:t] rows have cells[0] between t * 2048 and (t + 1) * 2048 - 8; rows after a device's total are unused. `bucket_counts`: each device's counts sum to at most 1024. For every index of vis, one tile receives exactly 512 rows from every device with that vis index; which tile is drawn.
All inputs are finite; a program needn't handle non-finite values.
Results may differ from the reference program's by a relative error of at most 0.008.
Values may be sent and summed in bfloat16 or wider, within the bound.
A program may use at most 64 MiB of HBM per device.

```python
import math
import jax
import jax.numpy as jnp
from jax import lax

COMPS = 2048
CHANS = 64
GRID = 8192
BAND = 128
ROWS_DEV = 1024
TAPS = 8
SLOT = 512
TILE_W = 2048
ROWS = 32768
N_VIS = 8
N_TILE = 4


def bucket_layout(key):
    folded = jax.random.fold_in(key, 7)
    device_total = N_VIS * N_TILE
    hottest = jax.random.randint(jax.random.fold_in(folded, 1), (N_VIS,), 0, N_TILE)
    others_most = (ROWS_DEV - SLOT) // (N_TILE - 1)
    others = jax.random.randint(jax.random.fold_in(folded, 2), (N_VIS, N_TILE, N_TILE), others_most // 4, others_most + 1)
    is_hottest = jnp.arange(N_TILE)[None, None, :] == hottest[:, None, None]
    return jnp.where(is_hottest, SLOT, others).reshape(device_total, N_TILE).astype(jnp.int32)


def draw_bucket_counts(key, part):
    return bucket_layout(key)


def draw_cells(key, part):
    folded = jax.random.fold_in(key, 7)
    device_total = N_VIS * N_TILE
    bucket_sizes = bucket_layout(key)
    bucket_ends = jnp.cumsum(bucket_sizes, axis=1)
    local_index = jnp.arange(ROWS_DEV, dtype=jnp.int32)
    tile_of = jnp.sum((local_index[None, :, None] >= bucket_ends[:, None, :]).astype(jnp.int32), axis=2)
    spare_tile = jax.random.randint(jax.random.fold_in(folded, 3), (device_total, ROWS_DEV), 0, N_TILE)
    tile_of = jnp.where(tile_of >= N_TILE, spare_tile, tile_of)
    within = jax.random.randint(jax.random.fold_in(folded, 4), (device_total, ROWS_DEV), 0, TILE_W - TAPS + 1)
    first_col = tile_of * TILE_W + within
    first_row = jax.random.randint(jax.random.fold_in(folded, 5), (device_total, ROWS_DEV), 0, BAND - TAPS + 1)
    return jnp.stack([first_col.reshape(-1), first_row.reshape(-1)]).astype(jnp.int32)


def plant(drawn, stream_key, smallest, top_value):
    longest = drawn.shape.index(max(drawn.shape))
    spots = []
    for shift in (0, 1):
        where = [jax.random.randint(jax.random.fold_in(stream_key, axis), (), 0, length) for axis, length in enumerate(drawn.shape)]
        where[longest] = (where[longest] + shift) % drawn.shape[longest]
        spots.append(tuple(where))
    return drawn.at[spots[0]].set(smallest).at[spots[1]].set(top_value)


def block_levels(key, shape, cuts, least, high):
    def one(dim, blocks):
        heights = jax.random.uniform(jax.random.fold_in(jax.random.fold_in(key, 6), dim), (blocks,), jnp.float32, least / len(cuts), high / len(cuts))
        return jnp.repeat(jnp.exp(heights), shape[dim] // blocks).reshape((-1,) + (1,) * (len(shape) - dim - 1))

    level = one(*cuts[0])
    for cut in cuts[1:]:
        level = level * one(*cut)
    return level


def normal_values(stream_key, extent, deviation, limit, pieces=(), kind=jnp.bfloat16):
    drawn = jax.random.normal(stream_key, extent, jnp.float32) * deviation
    if len(pieces) > 0:
        drawn = block_levels(stream_key, extent, pieces, -0.22, 0.18) * drawn
    return jnp.clip(drawn, min=-limit, max=limit).astype(kind)


def setup_inputs(seed: int = 0) -> dict:
    streams_of = jax.random.split(jax.random.key(seed), 8)
    return {
        "spectra": normal_values(streams_of[0], (CHANS, COMPS), (COMPS // 2) ** -0.5, 0.1875, ((1, 32),)),
        "positions": plant(jax.random.randint(streams_of[1], (2, COMPS), 0, GRID), jax.random.fold_in(streams_of[1], 1), 0, GRID - 1).astype(jnp.int32),
        "observed": normal_values(streams_of[2], (ROWS, 2 * CHANS), 1.0, 6.0, ((0, 32),)),
        "cells": draw_cells(jax.random.fold_in(streams_of[7], 71), 0),
        "fractions": jnp.clip(1.0 * jax.random.uniform(streams_of[4], (2, ROWS), jnp.float32) ** block_levels(streams_of[4], (2, ROWS), ((1, 32),), -0.2, 0.2), 0.0, 1.0),
        "bucket_counts": draw_bucket_counts(jax.random.fold_in(streams_of[7], 71), 0),
        "chan_weights": jnp.clip(jnp.exp(jax.random.uniform(streams_of[6], (CHANS,), jnp.float32, math.log(0.04), math.log(0.32))), 0.04, 0.32),
    }


def kernel_taps(offsets):
    taps_float = jnp.arange(TAPS, dtype=jnp.int32).astype(jnp.float32)
    shifted = (taps_float[None, :] - 3.0) - offsets[:, None]
    return jnp.exp(-0.5 * (shifted * shifted))


def reference(spectra, positions, observed, cells, fractions, bucket_counts, chan_weights):
    row_total = observed.shape[0]
    col_pixel = positions[0]
    row_pixel = positions[1]
    spectra_cols = spectra.T

    def predict_block(block_data):
        first_col, first_row, col_frac, row_frac = block_data
        turn_count = jnp.mod((first_col + 3)[:, None] * col_pixel[None, :] + (first_row + 3)[:, None] * row_pixel[None, :], GRID)
        phase_turns = turn_count.astype(jnp.float32) + col_frac[:, None] * col_pixel.astype(jnp.float32)[None, :] + row_frac[:, None] * row_pixel.astype(jnp.float32)[None, :]
        angles = phase_turns * (2.0 * math.pi / GRID)
        cosine = jnp.cos(angles).astype(jnp.bfloat16)
        sine_table = jnp.sin(angles).astype(jnp.bfloat16)
        real_part = jnp.dot(cosine, spectra_cols, preferred_element_type=jnp.float32)
        imag_part = -jnp.dot(sine_table, spectra_cols, preferred_element_type=jnp.float32)
        return jnp.concatenate([real_part, imag_part], axis=1)

    block_count = row_total // ROWS_DEV
    shaped = lambda array: array.reshape(block_count, ROWS_DEV)
    predicted = lax.map(predict_block, (shaped(cells[0]), shaped(cells[1]), shaped(fractions[0]), shaped(fractions[1])))
    predicted = predicted.reshape(row_total, 2 * CHANS)

    live_rows = jnp.sum(bucket_counts, axis=1)
    local_index = jnp.arange(ROWS_DEV, dtype=jnp.int32)
    row_live = (local_index[None, :] < live_rows[:, None]).reshape(row_total)
    residual = jnp.where(row_live[:, None], observed.astype(jnp.float32) - predicted, 0.0).astype(jnp.bfloat16)
    widened = residual.astype(jnp.float32)
    value_real = jnp.sum(widened[:, :CHANS] * chan_weights[None, :], axis=1)
    value_imag = jnp.sum(widened[:, CHANS:] * chan_weights[None, :], axis=1)

    row_kernel = kernel_taps(fractions[1])
    col_kernel = lax.optimization_barrier(kernel_taps(fractions[0]).astype(jnp.bfloat16)).astype(jnp.float32)
    left_real = lax.optimization_barrier((value_real[:, None] * row_kernel).astype(jnp.bfloat16)).astype(jnp.float32)
    left_imag = lax.optimization_barrier((value_imag[:, None] * row_kernel).astype(jnp.bfloat16)).astype(jnp.float32)

    taps_index = jnp.arange(TAPS, dtype=jnp.int32)
    row_index = jnp.broadcast_to(cells[1][:, None, None] + taps_index[None, :, None], (row_total, TAPS, TAPS))
    col_index = jnp.broadcast_to(cells[0][:, None, None] + taps_index[None, None, :], (row_total, TAPS, TAPS))
    contrib_real = left_real[:, :, None] * col_kernel[:, None, :]
    contrib_imag = left_imag[:, :, None] * col_kernel[:, None, :]
    grid_sum = jnp.zeros((BAND, 2, GRID), jnp.float32)
    grid_sum = grid_sum.at[row_index, 0, col_index].add(contrib_real)
    grid_sum = grid_sum.at[row_index, 1, col_index].add(contrib_imag)
    return residual, grid_sum
```

```python
import functools
import math

import jax
import jax.numpy as jnp
from jax import lax
from jax.experimental import pallas as pl
from jax.experimental.pallas import tpu as pltpu
from jax.sharding import PartitionSpec as P

GRID = 8192
BAND = 128
TAPS = 8
MESH = pl.DeviceIdType.MESH
VMEM_LIMIT = 60 * 1024 * 1024

COS = (0.9999992107823198, -19.73898035576402, 64.92865742103395, -85.2716215343041,
       58.79049212014272, -21.071105627647917)
SIN = (-6.28305408794423, 41.33112294859376, -81.36549856606159, 74.47097754866051,
       -32.768902424225836)
EXP_SCALE = -0.5 / math.log(2.0)


def position_features(positions):
    rows = []
    for axis in range(2):
        pixel = positions[axis]
        high = (pixel + 64) >> 7
        low = pixel - 128 * high
        high_wrapped = jnp.where(high >= 32, high - 64, high)
        rows += [low] * 5 + [128 * high_wrapped] + [128 * high] * 3
    return jnp.stack(rows).astype(jnp.bfloat16)


def gather_kernel(n_vis, n_tile, block_ref, out_ref, send_sems, recv_sems, pair_sems, own_sem):
    half = n_tile // 2
    count = n_vis * half
    vis = lax.axis_index("vis")
    tile = lax.axis_index("tile")
    core = tile % 2
    mine = vis * half + tile // 2

    def peer(step):
        place = (mine + step) % count
        return {"vis": place // half, "tile": (place % half) * 2 + core}

    partner = {"vis": vis, "tile": tile + 1 - 2 * core}
    barrier = pltpu.get_barrier_semaphore()

    @pl.loop(1, count)
    def _(step):
        pl.semaphore_signal(barrier, inc=1, device_id=peer(step), device_id_type=MESH)

    pl.semaphore_signal(barrier, inc=1, device_id=partner, device_id_type=MESH)
    own = pltpu.make_async_copy(block_ref, out_ref.at[core, mine], own_sem)
    own.start()
    pl.semaphore_wait(barrier, count)

    def send(step):
        return pltpu.make_async_remote_copy(
            src_ref=block_ref,
            dst_ref=out_ref.at[core, mine],
            send_sem=send_sems.at[step],
            recv_sem=recv_sems.at[step],
            device_id=peer(step),
            device_id_type=MESH,
        )

    @pl.loop(1, count)
    def _(step):
        send(step).start()

    own.wait()

    @pl.loop(1, count)
    def _(step):
        send(step).wait_recv()

    swap = pltpu.make_async_remote_copy(
        src_ref=out_ref.at[core],
        dst_ref=out_ref.at[core],
        send_sem=pair_sems.at[0],
        recv_sem=pair_sems.at[1],
        device_id=partner,
        device_id_type=MESH,
    )
    swap.start()

    @pl.loop(1, count)
    def _(step):
        send(step).wait_send()

    swap.wait()


def gather_components(block, n_vis, n_tile):
    count = n_vis * n_tile // 2
    return pl.pallas_call(
        functools.partial(gather_kernel, n_vis, n_tile),
        out_shape=jax.ShapeDtypeStruct((2, count) + block.shape, block.dtype),
        in_specs=[pl.BlockSpec(memory_space=pltpu.VMEM)],
        out_specs=pl.BlockSpec(memory_space=pltpu.VMEM),
        scratch_shapes=[
            pltpu.SemaphoreType.DMA((count,)),
            pltpu.SemaphoreType.DMA((count,)),
            pltpu.SemaphoreType.DMA((2,)),
            pltpu.SemaphoreType.DMA,
        ],
        compiler_params=pltpu.CompilerParams(
            collective_id=0, has_side_effects=True, vmem_limit_bytes=VMEM_LIMIT
        ),
        name="gather_components",
    )(block)


def place_rows(shape, first, rows):
    place = lax.broadcasted_iota(jnp.int32, shape, 0)
    table = jnp.zeros(shape, jnp.float32)
    for index, row in enumerate(rows):
        table = jnp.where(place == first + index, row, table)
    return table


def three_pieces(value):
    first = value.astype(jnp.bfloat16).astype(jnp.float32)
    rest = value - first
    second = rest.astype(jnp.bfloat16).astype(jnp.float32)
    return [first, second, rest - second]


def predict_kernel(
    channels, comps_ref, cells_ref, fractions_ref, observed_ref, counts_ref, weights_ref,
    residual_ref, packed_ref, left_ref,
):
    row_count = observed_ref.shape[0]
    comp_count = comps_ref.shape[0]
    tile_count, _, slot = packed_ref.shape
    row_block = min(128, row_count)
    comp_block = min(512, comp_count)

    factors = []
    for axis in range(2):
        cell = cells_ref[axis : axis + 1, :] + 3
        high = (cell + 32) >> 6
        low = (cell - 64 * high).astype(jnp.float32)
        high = jnp.where(high >= 64, high - 128, high)
        pieces = three_pieces(fractions_ref[axis : axis + 1, :])
        factors += [low, (64 * high).astype(jnp.float32)] + pieces + [low] + pieces
    table = place_rows((2 * channels, row_count), channels, factors) * (1.0 / GRID)
    left_ref[...] = table.T.astype(jnp.bfloat16)

    live = counts_ref[0, 0]
    for tile in range(1, tile_count):
        live = live + counts_ref[0, tile]

    @pl.loop(0, row_count // row_block)
    def _(step):
        start = pl.multiple_of(step * row_block, row_block)
        rows = pl.ds(start, row_block)
        left = left_ref[rows, :]
        real_part = jnp.zeros((row_block, 2 * channels), jnp.float32)
        imag_part = jnp.zeros((row_block, 2 * channels), jnp.float32)
        for first in range(0, comp_count, comp_block):
            comps = comps_ref[first : first + comp_block, :]
            turns = lax.dot_general(
                left, comps, (((1,), (1,)), ((), ())), preferred_element_type=jnp.float32
            )
            rest = turns - jnp.round(turns)
            square = rest * rest
            cosine = COS[-1] * square + COS[-2]
            for coefficient in COS[-3::-1]:
                cosine = cosine * square + coefficient
            sine = SIN[-1] * square + SIN[-2]
            for coefficient in SIN[-3::-1]:
                sine = sine * square + coefficient
            sine = sine * rest
            real_part += jnp.dot(
                cosine.astype(jnp.bfloat16), comps, preferred_element_type=jnp.float32
            )
            imag_part += jnp.dot(
                sine.astype(jnp.bfloat16), comps, preferred_element_type=jnp.float32
            )
        lane = lax.broadcasted_iota(jnp.int32, real_part.shape, 1)
        predicted = jnp.where(lane < channels, real_part, pltpu.roll(imag_part, channels, 1))
        row = start + lax.broadcasted_iota(jnp.int32, real_part.shape, 0)
        residual = jnp.where(row < live, observed_ref[rows, :].astype(jnp.float32) - predicted, 0.0)
        residual_ref[rows, :] = residual.astype(jnp.bfloat16)

    lane = lax.broadcasted_iota(jnp.int32, (1, 2 * channels), 1)
    weights = weights_ref[...]
    halves = [jnp.where(lane < channels, weights, 0.0), jnp.where(lane < channels, 0.0, weights)]
    weight_rows = [piece for half in halves for piece in three_pieces(half)]
    weight_table = place_rows((16, 2 * channels), 0, weight_rows).astype(jnp.bfloat16)
    sums = lax.dot_general(
        weight_table, residual_ref[...], (((1,), (1,)), ((), ())),
        preferred_element_type=jnp.float32,
    )
    data = place_rows(
        (8, row_count),
        0,
        [
            sums[0:1] + sums[1:2] + sums[2:3],
            sums[3:4] + sums[4:5] + sums[5:6],
            fractions_ref[0:1, :],
            fractions_ref[1:2, :],
            cells_ref[0:1, :].astype(jnp.float32),
            cells_ref[1:2, :].astype(jnp.float32),
        ],
    )
    begin = jnp.int32(0)
    place = lax.broadcasted_iota(jnp.int32, (8, slot), 0)
    index = lax.broadcasted_iota(jnp.int32, (8, slot), 1)
    for tile in range(tile_count):
        size = counts_ref[0, tile]
        moved = pltpu.roll(data, lax.rem(row_count - begin, row_count), 1)[:, :slot]
        packed_ref[tile] = jnp.where((place < 2) & (index >= size), 0.0, moved)
        begin = begin + size


def predict_rows(comps, cells, fractions, observed, bucket_counts, weights, slot):
    row_count, width = observed.shape
    tile_count = bucket_counts.shape[1]
    vmem = pl.BlockSpec(memory_space=pltpu.VMEM)
    return pl.pallas_call(
        functools.partial(predict_kernel, width // 2),
        out_shape=(
            jax.ShapeDtypeStruct(observed.shape, observed.dtype),
            jax.ShapeDtypeStruct((tile_count, 8, slot), jnp.float32),
        ),
        in_specs=[vmem, vmem, vmem, vmem, pl.BlockSpec(memory_space=pltpu.SMEM), vmem],
        out_specs=(vmem, vmem),
        scratch_shapes=[pltpu.VMEM((row_count, width), jnp.bfloat16)],
        compiler_params=pltpu.CompilerParams(vmem_limit_bytes=VMEM_LIMIT),
        name="predict_rows",
    )(comps, cells, fractions, observed, bucket_counts, weights)


def grid_kernel(
    n_vis, tile_width, data_ref, out_ref,
    rows_ref, left_ref, spread_ref, base_ref, sum_ref, own_ref, sent_ref, got_ref,
    send_sems, recv_sems,
):
    vis = lax.axis_index("vis")
    tile = lax.axis_index("tile")
    tile_count, _, slot = data_ref.shape
    owner_rows = sum_ref.shape[0] // n_vis
    chunk = sum_ref.shape[1]
    chunk_total = tile_width // chunk
    group = base_ref.shape[0]
    barrier = pltpu.get_barrier_semaphore()

    def peer(step):
        return {"vis": (vis + step) % n_vis}

    for step in range(1, n_vis):
        pl.semaphore_signal(barrier, inc=1, device_id=peer(step), device_id_type=MESH)

    for index in range(tile_count):
        rows_ref[:, index * slot : (index + 1) * slot] = data_ref[index]

    block = 2 * group
    for first in range(0, left_ref.shape[0], block):
        place = first + lax.broadcasted_iota(jnp.int32, (block, left_ref.shape[1]), 0)
        offset = (place >> 1).astype(jnp.float32) - 3.5 - rows_ref[5:6, :]
        shifted = offset - (rows_ref[3:4, :] - 0.5)
        weight = jnp.exp2(shifted * shifted * EXP_SCALE)
        value = jnp.where((place & 1) == 0, rows_ref[0:1, :], rows_ref[1:2, :])
        left_ref[first : first + block, :] = jnp.where(
            jnp.abs(offset) < 4.0, value * weight, 0.0
        ).astype(jnp.bfloat16)

    columns = rows_ref[4:5, :] - (tile * tile_width).astype(jnp.float32)
    lane_row = lax.broadcasted_iota(jnp.int32, base_ref.shape, 0).astype(jnp.float32)
    base_ref[...] = lane_row - 3.5 - columns

    def send(step, number):
        return pltpu.make_async_remote_copy(
            src_ref=sent_ref.at[(vis + step) % n_vis, number],
            dst_ref=got_ref.at[step, number],
            send_sem=send_sems.at[step, number],
            recv_sem=recv_sems.at[step, number],
            device_id=peer(step),
            device_id_type=MESH,
        )

    def compute(number):
        center = rows_ref[2:3, :] - 0.5
        start = number * chunk
        for first in range(0, chunk, group):
            offset = base_ref[...] + (start + first).astype(jnp.float32)
            shifted = offset - center
            weight = jnp.exp2(shifted * shifted * EXP_SCALE)
            spread_ref[first : first + group, :] = jnp.where(
                jnp.abs(offset) < 4.0, weight, 0.0
            ).astype(jnp.bfloat16)
        sum_ref[...] = lax.dot_general(
            left_ref[...], spread_ref[...], (((1,), (1,)), ((), ())),
            preferred_element_type=jnp.float32,
        )
        for owner in range(n_vis):
            sent_ref[owner, number] = sum_ref[
                owner * owner_rows : (owner + 1) * owner_rows, :
            ].astype(jnp.bfloat16)
        mine = pl.ds(pl.multiple_of(vis * owner_rows, owner_rows), owner_rows)
        own_ref[number] = sum_ref[mine, :]

    @pl.loop(0, chunk_total)
    def _(number):
        compute(number)

        @pl.when(number == 0)
        def _():
            pl.semaphore_wait(barrier, n_vis - 1)

        for step in range(1, n_vis):
            send(step, number).start()

    @pl.loop(0, chunk_total)
    def _(number):
        total = own_ref[number]
        for step in range(1, n_vis):
            send(step, number).wait_recv()
            total = total + got_ref[step, number].astype(jnp.float32)
        out_ref[:, pl.ds(pl.multiple_of(number * chunk, chunk), chunk)] = total

    @pl.loop(0, chunk_total)
    def _(number):
        for step in range(1, n_vis):
            send(step, number).wait_send()


def grid_rows(data, n_vis, tile_width):
    tile_count, _, slot = data.shape
    slots = tile_count * slot
    chunk = min(256, tile_width)
    chunk_total = tile_width // chunk
    owner_rows = 2 * BAND // n_vis
    vmem = pl.BlockSpec(memory_space=pltpu.VMEM)
    blocks = (n_vis, chunk_total, owner_rows, chunk)
    return pl.pallas_call(
        functools.partial(grid_kernel, n_vis, tile_width),
        out_shape=jax.ShapeDtypeStruct((owner_rows, tile_width), jnp.float32),
        in_specs=[vmem],
        out_specs=vmem,
        scratch_shapes=[
            pltpu.VMEM((8, slots), jnp.float32),
            pltpu.VMEM((2 * BAND, slots), jnp.bfloat16),
            pltpu.VMEM((chunk, slots), jnp.bfloat16),
            pltpu.VMEM((16, slots), jnp.float32),
            pltpu.VMEM((2 * BAND, chunk), jnp.float32),
            pltpu.VMEM((chunk_total, owner_rows, chunk), jnp.float32),
            pltpu.VMEM(blocks, jnp.bfloat16),
            pltpu.VMEM(blocks, jnp.bfloat16),
            pltpu.SemaphoreType.DMA((n_vis, chunk_total)),
            pltpu.SemaphoreType.DMA((n_vis, chunk_total)),
        ],
        compiler_params=pltpu.CompilerParams(
            collective_id=1, has_side_effects=True, vmem_limit_bytes=VMEM_LIMIT
        ),
        name="grid_rows",
    )(data)


def on_device(spectra, positions, observed, cells, fractions, bucket_counts, chan_weights):
    n_vis = lax.axis_size("vis")
    n_tile = lax.axis_size("tile")
    channels = chan_weights.shape[0]
    features = position_features(positions)
    spare = jnp.zeros((channels - features.shape[0], features.shape[1]), jnp.bfloat16)
    block = jnp.concatenate([spectra, features, spare], axis=0).T
    gathered = gather_components(block, n_vis, n_tile)
    comps = gathered.reshape(-1, 2 * channels)
    residual, packed = predict_rows(
        comps,
        cells,
        fractions,
        observed,
        bucket_counts,
        jnp.concatenate([chan_weights, chan_weights])[None, :],
        observed.shape[0] // 2,
    )
    packed = lax.all_to_all(packed, "tile", split_axis=0, concat_axis=0, tiled=True)
    share = grid_rows(packed, n_vis, GRID // n_tile)
    return (residual, share.reshape(BAND // n_vis, 2, GRID // n_tile))


def solution(mesh):
    placed = (
        P(None, ("vis", "tile")),
        P(None, ("vis", "tile")),
        P(("vis", "tile"), None),
        P(None, ("vis", "tile")),
        P(None, ("vis", "tile")),
        P(("vis", "tile"), None),
        P(),
    )
    return jax.shard_map(
        on_device,
        mesh=mesh,
        in_specs=placed,
        out_specs=(P(("vis", "tile"), None), P("vis", None, "tile")),
        check_vma=False,
    )
```

```python
import functools
import math

import jax
import jax.numpy as jnp
from jax import lax
from jax.experimental import pallas as pl
from jax.experimental.pallas import tpu as pltpu
from jax.sharding import PartitionSpec as P

GRID = 8192
BAND = 128
TAPS = 8
MESH = pl.DeviceIdType.MESH
VMEM_LIMIT = 60 * 1024 * 1024
LAG = 2

COS = (0.9999992107823198, -19.73898035576402, 64.92865742103395, -85.2716215343041,
       58.79049212014272, -21.071105627647917)
SIN = (-6.28305408794423, 41.33112294859376, -81.36549856606159, 74.47097754866051,
       -32.768902424225836)
EXP_SCALE = -0.5 / math.log(2.0)


def position_features(positions):
    rows = []
    for axis in range(2):
        pixel = positions[axis]
        high = (pixel + 64) >> 7
        low = pixel - 128 * high
        high_wrapped = jnp.where(high >= 32, high - 64, high)
        rows += [low] * 5 + [128 * high_wrapped] + [128 * high] * 3
    return jnp.stack(rows).astype(jnp.bfloat16)


def gather_kernel(n_vis, n_tile, block_ref, out_ref, send_sems, recv_sems, pair_sems, own_sem):
    half = n_tile // 2
    count = n_vis * half
    vis = lax.axis_index("vis")
    tile = lax.axis_index("tile")
    core = tile % 2
    mine = vis * half + tile // 2

    def peer(step):
        place = (mine + step) % count
        return {"vis": place // half, "tile": (place % half) * 2 + core}

    partner = {"vis": vis, "tile": tile + 1 - 2 * core}
    barrier = pltpu.get_barrier_semaphore()

    @pl.loop(1, count)
    def _(step):
        pl.semaphore_signal(barrier, inc=1, device_id=peer(step), device_id_type=MESH)

    pl.semaphore_signal(barrier, inc=1, device_id=partner, device_id_type=MESH)
    own = pltpu.make_async_copy(block_ref, out_ref.at[core, mine], own_sem)
    own.start()
    pl.semaphore_wait(barrier, count)

    def send(step):
        return pltpu.make_async_remote_copy(
            src_ref=block_ref,
            dst_ref=out_ref.at[core, mine],
            send_sem=send_sems.at[step],
            recv_sem=recv_sems.at[step],
            device_id=peer(step),
            device_id_type=MESH,
        )

    @pl.loop(1, count)
    def _(step):
        send(step).start()

    own.wait()

    @pl.loop(1, count)
    def _(step):
        send(step).wait_recv()

    swap = pltpu.make_async_remote_copy(
        src_ref=out_ref.at[core],
        dst_ref=out_ref.at[core],
        send_sem=pair_sems.at[0],
        recv_sem=pair_sems.at[1],
        device_id=partner,
        device_id_type=MESH,
    )
    swap.start()

    @pl.loop(1, count)
    def _(step):
        send(step).wait_send()

    swap.wait()


def gather_components(block, n_vis, n_tile):
    count = n_vis * n_tile // 2
    return pl.pallas_call(
        functools.partial(gather_kernel, n_vis, n_tile),
        out_shape=jax.ShapeDtypeStruct((2, count) + block.shape, block.dtype),
        in_specs=[pl.BlockSpec(memory_space=pltpu.VMEM)],
        out_specs=pl.BlockSpec(memory_space=pltpu.VMEM),
        scratch_shapes=[
            pltpu.SemaphoreType.DMA((count,)),
            pltpu.SemaphoreType.DMA((count,)),
            pltpu.SemaphoreType.DMA((2,)),
            pltpu.SemaphoreType.DMA,
        ],
        compiler_params=pltpu.CompilerParams(
            collective_id=0, has_side_effects=True, vmem_limit_bytes=VMEM_LIMIT
        ),
        name="gather_components",
    )(block)


def place_rows(shape, first, rows):
    place = lax.broadcasted_iota(jnp.int32, shape, 0)
    table = jnp.zeros(shape, jnp.float32)
    for index, row in enumerate(rows):
        table = jnp.where(place == first + index, row, table)
    return table


def three_pieces(value):
    first = value.astype(jnp.bfloat16).astype(jnp.float32)
    rest = value - first
    second = rest.astype(jnp.bfloat16).astype(jnp.float32)
    return [first, second, rest - second]


def predict_kernel(
    channels, comps_ref, cells_ref, fractions_ref, observed_ref, counts_ref, weights_ref,
    residual_ref, packed_ref, left_ref,
):
    row_count = observed_ref.shape[0]
    comp_count = comps_ref.shape[0]
    tile_count, _, slot = packed_ref.shape
    row_block = min(128, row_count)
    comp_block = min(512, comp_count)

    factors = []
    for axis in range(2):
        cell = cells_ref[axis : axis + 1, :] + 3
        high = (cell + 32) >> 6
        low = (cell - 64 * high).astype(jnp.float32)
        high = jnp.where(high >= 64, high - 128, high)
        pieces = three_pieces(fractions_ref[axis : axis + 1, :])
        factors += [low, (64 * high).astype(jnp.float32)] + pieces + [low] + pieces
    table = place_rows((2 * channels, row_count), channels, factors) * (1.0 / GRID)
    left_ref[...] = table.T.astype(jnp.bfloat16)

    live = counts_ref[0, 0]
    for tile in range(1, tile_count):
        live = live + counts_ref[0, tile]

    @pl.loop(0, row_count // row_block)
    def _(step):
        start = pl.multiple_of(step * row_block, row_block)
        rows = pl.ds(start, row_block)
        left = left_ref[rows, :]
        real_part = jnp.zeros((row_block, 2 * channels), jnp.float32)
        imag_part = jnp.zeros((row_block, 2 * channels), jnp.float32)
        for first in range(0, comp_count, comp_block):
            comps = comps_ref[first : first + comp_block, :]
            turns = lax.dot_general(
                left, comps, (((1,), (1,)), ((), ())), preferred_element_type=jnp.float32
            )
            rest = turns - jnp.round(turns)
            square = rest * rest
            cosine = COS[-1] * square + COS[-2]
            for coefficient in COS[-3::-1]:
                cosine = cosine * square + coefficient
            sine = SIN[-1] * square + SIN[-2]
            for coefficient in SIN[-3::-1]:
                sine = sine * square + coefficient
            sine = sine * rest
            real_part += jnp.dot(
                cosine.astype(jnp.bfloat16), comps, preferred_element_type=jnp.float32
            )
            imag_part += jnp.dot(
                sine.astype(jnp.bfloat16), comps, preferred_element_type=jnp.float32
            )
        lane = lax.broadcasted_iota(jnp.int32, real_part.shape, 1)
        predicted = jnp.where(lane < channels, real_part, pltpu.roll(imag_part, channels, 1))
        row = start + lax.broadcasted_iota(jnp.int32, real_part.shape, 0)
        residual = jnp.where(row < live, observed_ref[rows, :].astype(jnp.float32) - predicted, 0.0)
        residual_ref[rows, :] = residual.astype(jnp.bfloat16)

    lane = lax.broadcasted_iota(jnp.int32, (1, 2 * channels), 1)
    weights = weights_ref[...]
    halves = [jnp.where(lane < channels, weights, 0.0), jnp.where(lane < channels, 0.0, weights)]
    weight_rows = [piece for half in halves for piece in three_pieces(half)]
    weight_table = place_rows((16, 2 * channels), 0, weight_rows).astype(jnp.bfloat16)
    sums = lax.dot_general(
        weight_table, residual_ref[...], (((1,), (1,)), ((), ())),
        preferred_element_type=jnp.float32,
    )
    data = place_rows(
        (8, row_count),
        0,
        [
            sums[0:1] + sums[1:2] + sums[2:3],
            sums[3:4] + sums[4:5] + sums[5:6],
            fractions_ref[0:1, :],
            fractions_ref[1:2, :],
            cells_ref[0:1, :].astype(jnp.float32),
            cells_ref[1:2, :].astype(jnp.float32),
        ],
    )
    begin = jnp.int32(0)
    place = lax.broadcasted_iota(jnp.int32, (8, slot), 0)
    index = lax.broadcasted_iota(jnp.int32, (8, slot), 1)
    for tile in range(tile_count):
        size = counts_ref[0, tile]
        moved = pltpu.roll(data, lax.rem(row_count - begin, row_count), 1)[:, :slot]
        packed_ref[tile] = jnp.where((place < 2) & (index >= size), 0.0, moved)
        begin = begin + size


def predict_rows(comps, cells, fractions, observed, bucket_counts, weights, slot):
    row_count, width = observed.shape
    tile_count = bucket_counts.shape[1]
    vmem = pl.BlockSpec(memory_space=pltpu.VMEM)
    return pl.pallas_call(
        functools.partial(predict_kernel, width // 2),
        out_shape=(
            jax.ShapeDtypeStruct(observed.shape, observed.dtype),
            jax.ShapeDtypeStruct((tile_count, 8, slot), jnp.float32),
        ),
        in_specs=[vmem, vmem, vmem, vmem, pl.BlockSpec(memory_space=pltpu.SMEM), vmem],
        out_specs=(vmem, vmem),
        scratch_shapes=[pltpu.VMEM((row_count, width), jnp.bfloat16)],
        compiler_params=pltpu.CompilerParams(vmem_limit_bytes=VMEM_LIMIT),
        name="predict_rows",
    )(comps, cells, fractions, observed, bucket_counts, weights)


def grid_kernel(
    n_vis, tile_width, data_ref, out_ref,
    rows_ref, left_ref, spread_ref, base_ref, sum_ref, keep_ref, own_ref,
    pair_sent_ref, pair_got_ref, sent_ref, got_ref,
    pair_send_sems, pair_recv_sems, send_sems, recv_sems,
):
    vis = lax.axis_index("vis")
    tile = lax.axis_index("tile")
    tile_count, _, slot = data_ref.shape
    half = n_vis // 2
    owner_rows = own_ref.shape[1]
    chunk = own_ref.shape[2]
    chunk_total = tile_width // chunk
    group = base_ref.shape[0]
    side = vis % 2
    mine = vis // 2
    partner = {"vis": vis + 1 - 2 * side}
    barrier = pltpu.get_barrier_semaphore()

    def peer(step):
        return {"vis": ((mine + step) % half) * 2 + side}

    pl.semaphore_signal(barrier, inc=1, device_id=partner, device_id_type=MESH)
    for step in range(1, half):
        pl.semaphore_signal(barrier, inc=1, device_id=peer(step), device_id_type=MESH)

    for index in range(tile_count):
        rows_ref[:, index * slot : (index + 1) * slot] = data_ref[index]

    block = 2 * group
    for first in range(0, left_ref.shape[0], block):
        place = first + lax.broadcasted_iota(jnp.int32, (block, left_ref.shape[1]), 0)
        offset = (place >> 1).astype(jnp.float32) - 3.5 - rows_ref[5:6, :]
        shifted = offset - (rows_ref[3:4, :] - 0.5)
        weight = jnp.exp2(shifted * shifted * EXP_SCALE)
        value = jnp.where((place & 1) == 0, rows_ref[0:1, :], rows_ref[1:2, :])
        left_ref[first : first + block, :] = jnp.where(
            jnp.abs(offset) < 4.0, value * weight, 0.0
        ).astype(jnp.bfloat16)

    columns = rows_ref[4:5, :] - (tile * tile_width).astype(jnp.float32)
    lane_row = lax.broadcasted_iota(jnp.int32, base_ref.shape, 0).astype(jnp.float32)
    base_ref[...] = lane_row - 3.5 - columns

    def pair_send(number):
        return pltpu.make_async_remote_copy(
            src_ref=pair_sent_ref.at[number],
            dst_ref=pair_got_ref.at[number],
            send_sem=pair_send_sems.at[number],
            recv_sem=pair_recv_sems.at[number],
            device_id=partner,
            device_id_type=MESH,
        )

    def send(step, number):
        return pltpu.make_async_remote_copy(
            src_ref=sent_ref.at[step, number],
            dst_ref=got_ref.at[step, number],
            send_sem=send_sems.at[step, number],
            recv_sem=recv_sems.at[step, number],
            device_id=peer(step),
            device_id_type=MESH,
        )

    def compute(number):
        center = rows_ref[2:3, :] - 0.5
        start = number * chunk
        for first in range(0, chunk, group):
            offset = base_ref[...] + (start + first).astype(jnp.float32)
            shifted = offset - center
            weight = jnp.exp2(shifted * shifted * EXP_SCALE)
            spread_ref[first : first + group, :] = jnp.where(
                jnp.abs(offset) < 4.0, weight, 0.0
            ).astype(jnp.bfloat16)
        sums = lax.dot_general(
            left_ref[...], spread_ref[...], (((1,), (1,)), ((), ())),
            preferred_element_type=jnp.float32,
        )
        sum_ref[...] = sums.reshape(sum_ref.shape)
        for place in range(half):
            pair_sent_ref[number, place] = sum_ref[2 * place + 1 - side].astype(jnp.bfloat16)
            keep_ref[number, place] = sum_ref[2 * place + side]

    def combine(number):
        pair_send(number).wait_recv()
        own_ref[number] = keep_ref[number, mine] + pair_got_ref[number, mine].astype(jnp.float32)
        for step in range(1, half):
            place = (mine + step) % half
            total = keep_ref[number, place] + pair_got_ref[number, place].astype(jnp.float32)
            sent_ref[step, number] = total.astype(jnp.bfloat16)
        for step in range(1, half):
            send(step, number).start()

    @pl.loop(0, chunk_total)
    def _(number):
        compute(number)

        @pl.when(number == 0)
        def _():
            pl.semaphore_wait(barrier, half)

        pair_send(number).start()

        @pl.when(number >= LAG)
        def _():
            combine(number - LAG)

    @pl.loop(max(chunk_total - LAG, 0), chunk_total)
    def _(number):
        combine(number)

    @pl.loop(0, chunk_total)
    def _(number):
        total = own_ref[number]
        for step in range(1, half):
            send(step, number).wait_recv()
            total = total + got_ref[step, number].astype(jnp.float32)
        out_ref[:, pl.ds(pl.multiple_of(number * chunk, chunk), chunk)] = total

    @pl.loop(0, chunk_total)
    def _(number):
        pair_send(number).wait_send()
        for step in range(1, half):
            send(step, number).wait_send()


def grid_rows(data, n_vis, tile_width):
    tile_count, _, slot = data.shape
    slots = tile_count * slot
    chunk = min(256, tile_width)
    chunk_total = tile_width // chunk
    owner_rows = 2 * BAND // n_vis
    half = n_vis // 2
    vmem = pl.BlockSpec(memory_space=pltpu.VMEM)
    pair_blocks = (chunk_total, half, owner_rows, chunk)
    blocks = (half, chunk_total, owner_rows, chunk)
    return pl.pallas_call(
        functools.partial(grid_kernel, n_vis, tile_width),
        out_shape=jax.ShapeDtypeStruct((owner_rows, tile_width), jnp.float32),
        in_specs=[vmem],
        out_specs=vmem,
        scratch_shapes=[
            pltpu.VMEM((8, slots), jnp.float32),
            pltpu.VMEM((2 * BAND, slots), jnp.bfloat16),
            pltpu.VMEM((chunk, slots), jnp.bfloat16),
            pltpu.VMEM((16, slots), jnp.float32),
            pltpu.VMEM((n_vis, owner_rows, chunk), jnp.float32),
            pltpu.VMEM(pair_blocks, jnp.float32),
            pltpu.VMEM((chunk_total, owner_rows, chunk), jnp.float32),
            pltpu.VMEM(pair_blocks, jnp.bfloat16),
            pltpu.VMEM(pair_blocks, jnp.bfloat16),
            pltpu.VMEM(blocks, jnp.bfloat16),
            pltpu.VMEM(blocks, jnp.bfloat16),
            pltpu.SemaphoreType.DMA((chunk_total,)),
            pltpu.SemaphoreType.DMA((chunk_total,)),
            pltpu.SemaphoreType.DMA((half, chunk_total)),
            pltpu.SemaphoreType.DMA((half, chunk_total)),
        ],
        compiler_params=pltpu.CompilerParams(
            collective_id=1, has_side_effects=True, vmem_limit_bytes=VMEM_LIMIT
        ),
        name="grid_rows",
    )(data)


def on_device(spectra, positions, observed, cells, fractions, bucket_counts, chan_weights):
    n_vis = lax.axis_size("vis")
    n_tile = lax.axis_size("tile")
    channels = chan_weights.shape[0]
    features = position_features(positions)
    spare = jnp.zeros((channels - features.shape[0], features.shape[1]), jnp.bfloat16)
    block = jnp.concatenate([spectra, features, spare], axis=0).T
    gathered = gather_components(block, n_vis, n_tile)
    comps = gathered.reshape(-1, 2 * channels)
    residual, packed = predict_rows(
        comps,
        cells,
        fractions,
        observed,
        bucket_counts,
        jnp.concatenate([chan_weights, chan_weights])[None, :],
        observed.shape[0] // 2,
    )
    packed = lax.all_to_all(packed, "tile", split_axis=0, concat_axis=0, tiled=True)
    share = grid_rows(packed, n_vis, GRID // n_tile)
    return (residual, share.reshape(BAND // n_vis, 2, GRID // n_tile))


def solution(mesh):
    placed = (
        P(None, ("vis", "tile")),
        P(None, ("vis", "tile")),
        P(("vis", "tile"), None),
        P(None, ("vis", "tile")),
        P(None, ("vis", "tile")),
        P(("vis", "tile"), None),
        P(),
    )
    return jax.shard_map(
        on_device,
        mesh=mesh,
        in_specs=placed,
        out_specs=(P(("vis", "tile"), None), P("vis", None, "tile")),
        check_vma=False,
    )
```

```python
import functools
import math

import jax
import jax.numpy as jnp
from jax import lax
from jax.experimental import pallas as pl
from jax.experimental.pallas import tpu as pltpu
from jax.sharding import PartitionSpec as P

GRID = 8192
BAND = 128
TAPS = 8
MESH = pl.DeviceIdType.MESH
VMEM_LIMIT = 60 * 1024 * 1024
LAG = 2

COS = (0.9999992107823198, -19.73898035576402, 64.92865742103395, -85.2716215343041,
       58.79049212014272, -21.071105627647917)
SIN = (-6.28305408794423, 41.33112294859376, -81.36549856606159, 74.47097754866051,
       -32.768902424225836)
EXP_SCALE = -0.5 / math.log(2.0)


def position_features(positions):
    rows = []
    for axis in range(2):
        pixel = positions[axis]
        high = (pixel + 64) >> 7
        low = pixel - 128 * high
        high_wrapped = jnp.where(high >= 32, high - 64, high)
        rows += [low] * 5 + [128 * high_wrapped] + [128 * high] * 3
    return jnp.stack(rows).astype(jnp.bfloat16)


def gather_kernel(n_vis, n_tile, block_ref, out_ref, send_sems, recv_sems, pair_sems, own_sem):
    half = n_tile // 2
    count = n_vis * half
    vis = lax.axis_index("vis")
    tile = lax.axis_index("tile")
    core = tile % 2
    mine = vis * half + tile // 2

    def peer(step):
        place = (mine + step) % count
        return {"vis": place // half, "tile": (place % half) * 2 + core}

    partner = {"vis": vis, "tile": tile + 1 - 2 * core}
    barrier = pltpu.get_barrier_semaphore()

    @pl.loop(1, count)
    def _(step):
        pl.semaphore_signal(barrier, inc=1, device_id=peer(step), device_id_type=MESH)

    pl.semaphore_signal(barrier, inc=1, device_id=partner, device_id_type=MESH)
    own = pltpu.make_async_copy(block_ref, out_ref.at[core, mine], own_sem)
    own.start()
    pl.semaphore_wait(barrier, count)

    def send(step):
        return pltpu.make_async_remote_copy(
            src_ref=block_ref,
            dst_ref=out_ref.at[core, mine],
            send_sem=send_sems.at[step],
            recv_sem=recv_sems.at[step],
            device_id=peer(step),
            device_id_type=MESH,
        )

    @pl.loop(1, count)
    def _(step):
        send(step).start()

    own.wait()

    @pl.loop(1, count)
    def _(step):
        send(step).wait_recv()

    swap = pltpu.make_async_remote_copy(
        src_ref=out_ref.at[core],
        dst_ref=out_ref.at[core],
        send_sem=pair_sems.at[0],
        recv_sem=pair_sems.at[1],
        device_id=partner,
        device_id_type=MESH,
    )
    swap.start()

    @pl.loop(1, count)
    def _(step):
        send(step).wait_send()

    swap.wait()


def gather_components(block, n_vis, n_tile):
    count = n_vis * n_tile // 2
    return pl.pallas_call(
        functools.partial(gather_kernel, n_vis, n_tile),
        out_shape=jax.ShapeDtypeStruct((2, count) + block.shape, block.dtype),
        in_specs=[pl.BlockSpec(memory_space=pltpu.VMEM)],
        out_specs=pl.BlockSpec(memory_space=pltpu.VMEM),
        scratch_shapes=[
            pltpu.SemaphoreType.DMA((count,)),
            pltpu.SemaphoreType.DMA((count,)),
            pltpu.SemaphoreType.DMA((2,)),
            pltpu.SemaphoreType.DMA,
        ],
        compiler_params=pltpu.CompilerParams(
            collective_id=0, has_side_effects=True, vmem_limit_bytes=VMEM_LIMIT
        ),
        name="gather_components",
    )(block)


def place_rows(shape, first, rows):
    place = lax.broadcasted_iota(jnp.int32, shape, 0)
    table = jnp.zeros(shape, jnp.float32)
    for index, row in enumerate(rows):
        table = jnp.where(place == first + index, row, table)
    return table


def three_pieces(value):
    first = value.astype(jnp.bfloat16).astype(jnp.float32)
    rest = value - first
    second = rest.astype(jnp.bfloat16).astype(jnp.float32)
    return [first, second, rest - second]


def predict_kernel(
    channels, comps_ref, cells_ref, fractions_ref, observed_ref, counts_ref, weights_ref,
    residual_ref, packed_ref, left_ref,
):
    row_count = observed_ref.shape[0]
    comp_count = comps_ref.shape[0]
    tile_count, _, slot = packed_ref.shape
    row_block = min(128, row_count)
    comp_block = min(512, comp_count)

    factors = []
    for axis in range(2):
        cell = cells_ref[axis : axis + 1, :] + 3
        high = (cell + 32) >> 6
        low = (cell - 64 * high).astype(jnp.float32)
        high = jnp.where(high >= 64, high - 128, high)
        pieces = three_pieces(fractions_ref[axis : axis + 1, :])
        factors += [low, (64 * high).astype(jnp.float32)] + pieces + [low] + pieces
    table = place_rows((2 * channels, row_count), channels, factors) * (1.0 / GRID)
    left_ref[...] = table.T.astype(jnp.bfloat16)

    live = counts_ref[0, 0]
    for tile in range(1, tile_count):
        live = live + counts_ref[0, tile]

    @pl.loop(0, row_count // row_block)
    def _(step):
        start = pl.multiple_of(step * row_block, row_block)
        rows = pl.ds(start, row_block)
        left = left_ref[rows, :]
        real_part = jnp.zeros((row_block, 2 * channels), jnp.float32)
        imag_part = jnp.zeros((row_block, 2 * channels), jnp.float32)
        for first in range(0, comp_count, comp_block):
            comps = comps_ref[first : first + comp_block, :]
            turns = lax.dot_general(
                left, comps, (((1,), (1,)), ((), ())), preferred_element_type=jnp.float32
            )
            rest = turns - jnp.round(turns)
            square = rest * rest
            cosine = COS[-1] * square + COS[-2]
            for coefficient in COS[-3::-1]:
                cosine = cosine * square + coefficient
            sine = SIN[-1] * square + SIN[-2]
            for coefficient in SIN[-3::-1]:
                sine = sine * square + coefficient
            sine = sine * rest
            real_part += jnp.dot(
                cosine.astype(jnp.bfloat16), comps, preferred_element_type=jnp.float32
            )
            imag_part += jnp.dot(
                sine.astype(jnp.bfloat16), comps, preferred_element_type=jnp.float32
            )
        lane = lax.broadcasted_iota(jnp.int32, real_part.shape, 1)
        predicted = jnp.where(lane < channels, real_part, pltpu.roll(imag_part, channels, 1))
        row = start + lax.broadcasted_iota(jnp.int32, real_part.shape, 0)
        residual = jnp.where(row < live, observed_ref[rows, :].astype(jnp.float32) - predicted, 0.0)
        residual_ref[rows, :] = residual.astype(jnp.bfloat16)

    lane = lax.broadcasted_iota(jnp.int32, (1, 2 * channels), 1)
    weights = weights_ref[...]
    halves = [jnp.where(lane < channels, weights, 0.0), jnp.where(lane < channels, 0.0, weights)]
    weight_rows = [piece for half in halves for piece in three_pieces(half)]
    weight_table = place_rows((16, 2 * channels), 0, weight_rows).astype(jnp.bfloat16)
    sums = lax.dot_general(
        weight_table, residual_ref[...], (((1,), (1,)), ((), ())),
        preferred_element_type=jnp.float32,
    )
    data = place_rows(
        (8, row_count),
        0,
        [
            sums[0:1] + sums[1:2] + sums[2:3],
            sums[3:4] + sums[4:5] + sums[5:6],
            fractions_ref[0:1, :],
            fractions_ref[1:2, :],
            cells_ref[0:1, :].astype(jnp.float32),
            cells_ref[1:2, :].astype(jnp.float32),
        ],
    )
    begin = jnp.int32(0)
    place = lax.broadcasted_iota(jnp.int32, (8, slot), 0)
    index = lax.broadcasted_iota(jnp.int32, (8, slot), 1)
    for tile in range(tile_count):
        size = counts_ref[0, tile]
        moved = pltpu.roll(data, lax.rem(row_count - begin, row_count), 1)[:, :slot]
        packed_ref[tile] = jnp.where((place < 2) & (index >= size), 0.0, moved)
        begin = begin + size


def predict_rows(comps, cells, fractions, observed, bucket_counts, weights, slot):
    row_count, width = observed.shape
    tile_count = bucket_counts.shape[1]
    vmem = pl.BlockSpec(memory_space=pltpu.VMEM)
    return pl.pallas_call(
        functools.partial(predict_kernel, width // 2),
        out_shape=(
            jax.ShapeDtypeStruct(observed.shape, observed.dtype),
            jax.ShapeDtypeStruct((tile_count, 8, slot), jnp.float32),
        ),
        in_specs=[vmem, vmem, vmem, vmem, pl.BlockSpec(memory_space=pltpu.SMEM), vmem],
        out_specs=(vmem, vmem),
        scratch_shapes=[pltpu.VMEM((row_count, width), jnp.bfloat16)],
        compiler_params=pltpu.CompilerParams(vmem_limit_bytes=VMEM_LIMIT),
        name="predict_rows",
    )(comps, cells, fractions, observed, bucket_counts, weights)


def grid_kernel(
    n_vis, tile_width, data_ref, out_ref,
    rows_ref, left_ref, spread_ref, base_ref, sum_ref, keep_ref, own_ref,
    pair_sent_ref, pair_got_ref, sent_ref, got_ref,
    pair_send_sems, pair_recv_sems, send_sems, recv_sems,
    slots_ref, slot_send_sems, slot_recv_sems,
):
    vis = lax.axis_index("vis")
    tile = lax.axis_index("tile")
    tile_count, _, slot = data_ref.shape
    half = n_vis // 2
    owner_rows = own_ref.shape[1]
    chunk = own_ref.shape[2]
    chunk_total = tile_width // chunk
    group = base_ref.shape[0]
    side = vis % 2
    mine = vis // 2
    partner = {"vis": vis + 1 - 2 * side}
    barrier = pltpu.get_barrier_semaphore()

    def peer(step):
        return {"vis": ((mine + step) % half) * 2 + side}

    pl.semaphore_signal(barrier, inc=1, device_id=partner, device_id_type=MESH)
    for step in range(1, half):
        pl.semaphore_signal(barrier, inc=1, device_id=peer(step), device_id_type=MESH)

    def owner(step):
        return (tile + step) % tile_count

    def slot_send(step):
        return pltpu.make_async_remote_copy(
            src_ref=data_ref.at[owner(step)],
            dst_ref=slots_ref.at[step],
            send_sem=slot_send_sems.at[step],
            recv_sem=slot_recv_sems.at[step],
            device_id={"tile": owner(step)},
            device_id_type=MESH,
        )

    for step in range(1, tile_count):
        pl.semaphore_signal(
            barrier, inc=1, device_id={"tile": owner(step)}, device_id_type=MESH
        )
    pl.semaphore_wait(barrier, half + tile_count - 1)
    for step in range(1, tile_count):
        slot_send(step).start()
    rows_ref[:, :slot] = data_ref[tile]
    for step in range(1, tile_count):
        slot_send(step).wait_recv()
        rows_ref[:, step * slot : (step + 1) * slot] = slots_ref[step]

    block = 2 * group
    for first in range(0, left_ref.shape[0], block):
        place = first + lax.broadcasted_iota(jnp.int32, (block, left_ref.shape[1]), 0)
        offset = (place >> 1).astype(jnp.float32) - 3.5 - rows_ref[5:6, :]
        shifted = offset - (rows_ref[3:4, :] - 0.5)
        weight = jnp.exp2(shifted * shifted * EXP_SCALE)
        value = jnp.where((place & 1) == 0, rows_ref[0:1, :], rows_ref[1:2, :])
        left_ref[first : first + block, :] = jnp.where(
            jnp.abs(offset) < 4.0, value * weight, 0.0
        ).astype(jnp.bfloat16)

    columns = rows_ref[4:5, :] - (tile * tile_width).astype(jnp.float32)
    lane_row = lax.broadcasted_iota(jnp.int32, base_ref.shape, 0).astype(jnp.float32)
    base_ref[...] = lane_row - 3.5 - columns

    def pair_send(number):
        return pltpu.make_async_remote_copy(
            src_ref=pair_sent_ref.at[number],
            dst_ref=pair_got_ref.at[number],
            send_sem=pair_send_sems.at[number],
            recv_sem=pair_recv_sems.at[number],
            device_id=partner,
            device_id_type=MESH,
        )

    def send(step, number):
        return pltpu.make_async_remote_copy(
            src_ref=sent_ref.at[step, number],
            dst_ref=got_ref.at[step, number],
            send_sem=send_sems.at[step, number],
            recv_sem=recv_sems.at[step, number],
            device_id=peer(step),
            device_id_type=MESH,
        )

    def compute(number):
        center = rows_ref[2:3, :] - 0.5
        start = number * chunk
        for first in range(0, chunk, group):
            offset = base_ref[...] + (start + first).astype(jnp.float32)
            shifted = offset - center
            weight = jnp.exp2(shifted * shifted * EXP_SCALE)
            spread_ref[first : first + group, :] = jnp.where(
                jnp.abs(offset) < 4.0, weight, 0.0
            ).astype(jnp.bfloat16)
        sums = lax.dot_general(
            left_ref[...], spread_ref[...], (((1,), (1,)), ((), ())),
            preferred_element_type=jnp.float32,
        )
        sum_ref[...] = sums.reshape(sum_ref.shape)
        for place in range(half):
            pair_sent_ref[number, place] = sum_ref[2 * place + 1 - side].astype(jnp.bfloat16)
            keep_ref[number, place] = sum_ref[2 * place + side]

    def combine(number):
        pair_send(number).wait_recv()
        own_ref[number] = keep_ref[number, mine] + pair_got_ref[number, mine].astype(jnp.float32)
        for step in range(1, half):
            place = (mine + step) % half
            total = keep_ref[number, place] + pair_got_ref[number, place].astype(jnp.float32)
            sent_ref[step, number] = total.astype(jnp.bfloat16)
        for step in range(1, half):
            send(step, number).start()

    @pl.loop(0, chunk_total)
    def _(number):
        compute(number)

        pair_send(number).start()

        @pl.when(number >= LAG)
        def _():
            combine(number - LAG)

    @pl.loop(max(chunk_total - LAG, 0), chunk_total)
    def _(number):
        combine(number)

    @pl.loop(0, chunk_total)
    def _(number):
        total = own_ref[number]
        for step in range(1, half):
            send(step, number).wait_recv()
            total = total + got_ref[step, number].astype(jnp.float32)
        out_ref[:, pl.ds(pl.multiple_of(number * chunk, chunk), chunk)] = total

    for step in range(1, tile_count):
        slot_send(step).wait_send()

    @pl.loop(0, chunk_total)
    def _(number):
        pair_send(number).wait_send()
        for step in range(1, half):
            send(step, number).wait_send()


def grid_rows(data, n_vis, tile_width):
    tile_count, _, slot = data.shape
    slots = tile_count * slot
    chunk = min(256, tile_width)
    chunk_total = tile_width // chunk
    owner_rows = 2 * BAND // n_vis
    half = n_vis // 2
    vmem = pl.BlockSpec(memory_space=pltpu.VMEM)
    pair_blocks = (chunk_total, half, owner_rows, chunk)
    blocks = (half, chunk_total, owner_rows, chunk)
    return pl.pallas_call(
        functools.partial(grid_kernel, n_vis, tile_width),
        out_shape=jax.ShapeDtypeStruct((owner_rows, tile_width), jnp.float32),
        in_specs=[vmem],
        out_specs=vmem,
        scratch_shapes=[
            pltpu.VMEM((8, slots), jnp.float32),
            pltpu.VMEM((2 * BAND, slots), jnp.bfloat16),
            pltpu.VMEM((chunk, slots), jnp.bfloat16),
            pltpu.VMEM((16, slots), jnp.float32),
            pltpu.VMEM((n_vis, owner_rows, chunk), jnp.float32),
            pltpu.VMEM(pair_blocks, jnp.float32),
            pltpu.VMEM((chunk_total, owner_rows, chunk), jnp.float32),
            pltpu.VMEM(pair_blocks, jnp.bfloat16),
            pltpu.VMEM(pair_blocks, jnp.bfloat16),
            pltpu.VMEM(blocks, jnp.bfloat16),
            pltpu.VMEM(blocks, jnp.bfloat16),
            pltpu.SemaphoreType.DMA((chunk_total,)),
            pltpu.SemaphoreType.DMA((chunk_total,)),
            pltpu.SemaphoreType.DMA((half, chunk_total)),
            pltpu.SemaphoreType.DMA((half, chunk_total)),
            pltpu.VMEM(data.shape, jnp.float32),
            pltpu.SemaphoreType.DMA((tile_count,)),
            pltpu.SemaphoreType.DMA((tile_count,)),
        ],
        compiler_params=pltpu.CompilerParams(
            collective_id=1, has_side_effects=True, vmem_limit_bytes=VMEM_LIMIT
        ),
        name="grid_rows",
    )(data)


def on_device(spectra, positions, observed, cells, fractions, bucket_counts, chan_weights):
    n_vis = lax.axis_size("vis")
    n_tile = lax.axis_size("tile")
    channels = chan_weights.shape[0]
    features = position_features(positions)
    spare = jnp.zeros((channels - features.shape[0], features.shape[1]), jnp.bfloat16)
    block = jnp.concatenate([spectra, features, spare], axis=0).T
    gathered = gather_components(block, n_vis, n_tile)
    comps = gathered.reshape(-1, 2 * channels)
    residual, packed = predict_rows(
        comps,
        cells,
        fractions,
        observed,
        bucket_counts,
        jnp.concatenate([chan_weights, chan_weights])[None, :],
        observed.shape[0] // 2,
    )
    share = grid_rows(packed, n_vis, GRID // n_tile)
    return (residual, share.reshape(BAND // n_vis, 2, GRID // n_tile))


def solution(mesh):
    placed = (
        P(None, ("vis", "tile")),
        P(None, ("vis", "tile")),
        P(("vis", "tile"), None),
        P(None, ("vis", "tile")),
        P(None, ("vis", "tile")),
        P(("vis", "tile"), None),
        P(),
    )
    return jax.shard_map(
        on_device,
        mesh=mesh,
        in_specs=placed,
        out_specs=(P(("vis", "tile"), None), P("vis", None, "tile")),
        check_vma=False,
    )
```
